32 devices in a mesh: site: 2 (over y), handler: 4 (over x, core), worker: 4 (over z).
Axes of the slice: x: 2, y: 2, z: 4, core: 2. Of those that a mesh axis runs over, the one named last changes fastest.
Arguments:
- sgt: bfloat16 [2048, 6, 3, 1024], P(('site', 'handler', 'worker')), parts along dimension 0, may hold values from -6 to 6
- mechanism: bfloat16 [6, 1024], P(None, ('handler', 'worker')), may hold values from -2.5 to 2.5
- req_owner: int32 [1024, 1], P(('site', 'handler', 'worker')), parts along dimension 0, may hold values from 0 to 15; in each aligned block of 32 rows (0 to 31, 32 to 63, ...) at most 4 rows name the same one
- req_local: int32 [1024], P(('site', 'handler', 'worker')), parts along dimension 0, may hold values from 0 to 31
- slip: bfloat16 [1024, 64, 128], P(('site', 'handler', 'worker')), parts along dimension 0, may hold values from 0 to 0.029907227
Outputs:
- seismograms: float32 [32, 64, 3, 1024], P(('site', 'handler'), 'worker'), parts along dimension 0
The draws below stay inside these ranges and needn't reach their ends.
There are 2 independent parts, one for each index of `site`. The reference program is written for one: setup_inputs(seed, part) draws one part's arguments, and reference() takes and returns one part's arrays. A program takes and returns all parts, laid end to end along the dimension named above; an argument that names none is the same for every part. Nothing has to cross between parts.
Inputs may be any that keep to these rules, and one draw needn't show every extreme that they name: `req_owner`: among the 32 requests of one device no owner is named more than 4 times, and in every draw some device names some owner exactly 4 times; every owner is named somewhere.
All inputs are finite; a program needn't handle non-finite values.
Results may differ from the reference program's by a relative error of at most 0.0029.
Values may be sent and summed in bfloat16 or wider, within the bound.
A program may use at most 128 MiB of HBM per device.

```python
import math
import jax
import jax.numpy as jnp
import numpy as np
from jax import lax

SAMPLES = 1024
VARS = 64
TAPS = 64
BLK = 2
RUP_SLOTS = 4
REQ = 32
PTS_DEV = 64
POINTS = 1024
REQUESTS = 512
RUPTURES = 16
CAP = 4
N_HANDLER = 4
N_WORKER = 4


def with_ends(drawn, key, smallest, largest):
    shape = drawn.shape
    spot = [jax.random.randint(jax.random.fold_in(key, axis), (), 0, shape[axis]) for axis in range(len(shape))]
    drawn = drawn.at[tuple(spot)].set(smallest)
    longest = shape.index(max(shape))
    spot[longest] = (spot[longest] + 1) % shape[longest]
    return drawn.at[tuple(spot)].set(largest)


def block_levels(key, dims, split, least, top_value):
    def one(axis_at, parts):
        heights = jax.random.uniform(jax.random.fold_in(jax.random.fold_in(key, 6), axis_at), (parts,), jnp.float32, least / len(split), top_value / len(split))
        return jnp.repeat(jnp.exp(heights), dims[axis_at] // parts).reshape((-1,) + (1,) * (len(dims) - axis_at - 1))

    loudness = one(*split[0])
    for cut in split[1:]:
        loudness = loudness * one(*cut)
    return loudness


def deal_out(key, own, number, rows, amount, top, limit, slope):
    sequence = jax.random.permutation(key, amount)
    packed, usual = portions_of(amount, rows * top, limit, slope, True), portions_of(amount, rows * top, limit, slope, False)
    places = jnp.arange(amount)

    def named(lengths, turn):
        used = int((lengths > 0).sum())
        fixed = max(1, used // 4)
        shifted = fixed + (places - fixed + turn * (used - fixed)) % max(1, amount - fixed)
        return jnp.zeros((amount,), jnp.int32).at[sequence[jnp.where(places < fixed, places, shifted)]].set(jnp.asarray(lengths, jnp.int32))

    lengths = jnp.where(number % 4 == 0, named(packed, number // 4), named(usual, number - number // 4 - 1))
    mixed = jax.random.permutation(jax.random.fold_in(own, 3), amount)
    donor, sink = mixed[0:amount // 2 * 2:2], mixed[1:amount // 2 * 2:2]
    margin = jnp.minimum(lengths[donor] - 1, limit - lengths[sink]) // 2
    margin = jnp.where((donor == sequence[0]) | (sink == sequence[0]) | (lengths[sink] == 0), 0, jnp.maximum(margin, 0))
    shifted = jax.random.randint(jax.random.fold_in(own, 4), (amount // 2,), 0, 1 << 20) % (margin + 1)
    lengths = lengths.at[donor].add(-shifted).at[sink].add(shifted)
    members = jnp.searchsorted(jnp.cumsum(lengths), jnp.arange(rows * top), side="right").astype(jnp.int32)
    table = members.reshape(top, rows).T
    table = table[jax.random.permutation(jax.random.fold_in(own, 1), rows)]
    turn = jax.random.randint(jax.random.fold_in(own, 2), (rows, 1), 0, top)
    return jnp.take_along_axis(table, (jnp.arange(top)[None, :] + turn) % top, axis=1)


def portions_of(amount, total, reach, lean, full):
    loads = [(1 << 20) // math.isqrt(standing ** lean) + 1 for standing in range(1, amount + 1)]
    largest = reach if full else min(reach, max(-(-total // amount), total * loads[0] // sum(loads)))
    least = 1 if total - largest >= amount - 1 else 0
    given, spare = [largest] + [least] * (amount - 1), total - largest - least * (amount - 1)
    while spare > 0:
        free = [i for i in range(1, amount) if given[i] < largest] or [i for i in range(1, amount) if given[i] < reach]
        pool, left = sum([loads[i] for i in free]), spare
        for i in free:
            more = min(reach - given[i], max(1, left * loads[i] // pool), spare)
            given[i] = given[i] + more
            spare = spare - more
    return np.array(given)


def gaussian(key, dims, spread, most, split=(), dtype=jnp.bfloat16):
    drawn = spread * jax.random.normal(key, dims, jnp.float32)
    if split:
        drawn = drawn * block_levels(key, dims, split, -0.22, 0.18)
    return jnp.clip(drawn, -most, most).astype(dtype)


def setup_inputs(seed: int = 0, part: int = 0) -> dict:
    seeds = jax.random.split(jax.random.key(seed), 6)
    own_keys = jax.random.split(jax.random.fold_in(seeds[5], part), 6)
    sgt = gaussian(own_keys[0], (POINTS, 6, 3, SAMPLES), 1.0, 6.0, ((0, 16),))
    mechanism = gaussian(seeds[1], (6, POINTS), 6 ** -0.5, 2.5, ((1, 16),))
    req_owner_keys = jax.random.split(jax.random.fold_in(own_keys[2], 1), REQUESTS // REQ)
    req_owner_turns = jax.random.permutation(jax.random.fold_in(own_keys[2], 3), REQUESTS // REQ)
    req_owner = jax.vmap(lambda own, number: deal_out(jax.random.fold_in(own_keys[2], 2), own, number, REQ, N_HANDLER * N_WORKER, 1, CAP, 2))(req_owner_keys, req_owner_turns).reshape((REQUESTS, 1))
    req_local = with_ends(jax.random.randint(own_keys[3], (REQUESTS,), 0, PTS_DEV // BLK), jax.random.fold_in(own_keys[3], 1), 0, (PTS_DEV // BLK) - 1).astype(jnp.int32)
    slip = jnp.clip(0.029907227 * jax.random.uniform(own_keys[4], (REQUESTS, VARS, BLK * TAPS), jnp.float32) ** block_levels(own_keys[4], (REQUESTS, VARS, BLK * TAPS), ((0, 16),), -0.2, 0.2), 0.0, 0.029907227).astype(jnp.bfloat16)
    return dict(sgt=sgt, mechanism=mechanism, req_owner=req_owner, req_local=req_local, slip=slip)


def combine_points(sgt, mechanism):
    total = mechanism[0].astype(jnp.float32)[:, None, None] * sgt[:, 0].astype(jnp.float32)
    for comp in range(1, 6):
        total = total + mechanism[comp].astype(jnp.float32)[:, None, None] * sgt[:, comp].astype(jnp.float32)
    return total.astype(jnp.bfloat16)


def shifted_blocks(green):
    samples = green.shape[-1]
    padded = jnp.pad(green, ((0, 0), (0, 0), (0, 0), (TAPS, 0)))
    return jnp.stack([padded[..., TAPS - lag:TAPS - lag + samples] for lag in range(TAPS)], axis=2)


def device_partial(blocks, slip_rows):
    rows = blocks.shape[0] // RUP_SLOTS
    samples = blocks.shape[-1]
    outputs = []
    for slot in range(RUP_SLOTS):
        stacked = shifted_blocks(blocks[slot * rows:(slot + 1) * rows])
        right = stacked.reshape(rows * BLK * TAPS, 3 * samples)
        left = jnp.transpose(slip_rows[slot * rows:(slot + 1) * rows], (1, 0, 2)).reshape(VARS, rows * BLK * TAPS)
        outputs.append(jnp.dot(left, right, preferred_element_type=jnp.float32).reshape(VARS, 3, samples))
    return jnp.stack(outputs, axis=0)


def reference(sgt, mechanism, req_owner, req_local, slip):
    devices_part = N_HANDLER * N_WORKER
    per_owner = PTS_DEV // BLK
    green = combine_points(sgt, mechanism)
    green_blocks = green.reshape(POINTS // BLK, BLK, 3, SAMPLES)
    block_ids = (req_owner[:, 0] * per_owner + req_local).astype(jnp.int32)
    block_ids = block_ids.reshape(devices_part, REQ)
    slip_dev = slip.reshape(devices_part, REQ, VARS, BLK * TAPS)

    def one_device(pair):
        ids, slip_rows = pair
        return device_partial(green_blocks[ids], slip_rows)

    partial_value = lax.map(one_device, (block_ids, slip_dev))
    partial_value = partial_value.reshape(N_HANDLER, N_WORKER, RUP_SLOTS, VARS, 3, SAMPLES)
    return jnp.sum(partial_value, axis=1).reshape(RUPTURES, VARS, 3, SAMPLES)
```

```python
import functools
import jax
import jax.numpy as jnp
from jax import lax
from jax.experimental import pallas as pl
from jax.experimental.pallas import tpu as pltpu
from jax.sharding import PartitionSpec as P

TAPS = 64
BLK = 2
RUP_SLOTS = 4
OUTER = 4
INNER = TAPS // OUTER


def combine_points(sgt, mechanism):
    total = mechanism[0].astype(jnp.float32)[:, None, None] * sgt[:, 0].astype(jnp.float32)
    for comp in range(1, 6):
        total = total + mechanism[comp].astype(jnp.float32)[:, None, None] * sgt[:, comp].astype(
            jnp.float32
        )
    return total.astype(jnp.bfloat16)


def conv_kernel(rows, variations, samples, workers, blk_ref, slip_ref, out_ref, shift_ref):
    depth = INNER * BLK * rows
    share = variations // workers
    lane = lax.broadcasted_iota(jnp.int32, (BLK * rows, samples), 1)
    wide = lax.broadcasted_iota(jnp.int32, (variations, samples), 1)

    def slot_step(slot, carry):
        left = jnp.concatenate(
            [slip_ref[slot, :, a * depth : (a + 1) * depth] for a in range(OUTER)], axis=0
        )
        for k in range(3):
            x = jnp.concatenate(
                [
                    blk_ref[slot, :, (i * 3 + k) * samples : (i * 3 + k + 1) * samples]
                    for i in range(BLK)
                ],
                axis=0,
            ).astype(jnp.float32)
            for b in range(INNER):
                moved = x if b == 0 else jnp.where(lane >= b, pltpu.roll(x, b, 1), 0.0)
                shift_ref[b * BLK * rows : (b + 1) * BLK * rows, :] = moved.astype(jnp.bfloat16)
            y = jnp.dot(left, shift_ref[...], preferred_element_type=jnp.float32)
            total = y[:variations]
            for a in range(1, OUTER):
                part = pltpu.roll(y[a * variations : (a + 1) * variations], a * INNER, 1)
                total = total + jnp.where(wide >= a * INNER, part, 0.0)
            total = total.astype(jnp.bfloat16)
            for w in range(workers):
                out_ref[w, slot, k] = total[w * share : (w + 1) * share]
        return carry

    lax.fori_loop(0, RUP_SLOTS, slot_step, 0)


def local(workers, sgt, mechanism, req_owner, req_local, slip):
    peers = lax.axis_size(("handler", "worker"))
    samples = sgt.shape[-1]
    blocks_here = sgt.shape[0] // BLK
    requests = req_local.shape[0]
    rows = requests // RUP_SLOTS
    variations = slip.shape[1]
    capacity = max(2, (2 * requests + peers - 1) // peers)
    owner = req_owner[:, 0]
    order = jnp.arange(requests)
    same = (owner[:, None] == owner[None, :]) & (order[:, None] > order[None, :])
    position = owner * capacity + jnp.sum(same.astype(jnp.int32), axis=1)
    places = jnp.arange(peers * capacity, dtype=jnp.int32)
    table = jnp.sum(
        jnp.where(position[:, None] == places[None, :], req_local[:, None], 0), axis=0
    )
    asked = lax.all_to_all(
        table.reshape(peers, capacity),
        ("handler", "worker"),
        split_axis=0,
        concat_axis=0,
        tiled=True,
    )
    green_here = combine_points(sgt, mechanism).reshape(blocks_here, BLK * 3 * samples)
    chosen = green_here[asked.reshape(-1)].reshape(peers, capacity * BLK * 3 * samples)
    chosen = chosen.reshape(peers, capacity, BLK * 3 * samples)
    arrived = lax.all_to_all(
        chosen, ("handler", "worker"), split_axis=0, concat_axis=0, tiled=True
    )
    blocks = arrived.reshape(peers * capacity, BLK * 3 * samples)[position]
    blocks = blocks.reshape(RUP_SLOTS, rows, BLK * 3 * samples)

    full = rows * BLK * TAPS
    src = jnp.arange(full, dtype=jnp.int32)
    dst_of = (
        (src % TAPS) * (BLK * rows) + (src // TAPS) % BLK * rows + src // (TAPS * BLK)
    )
    move = (dst_of[:, None] == src[None, :]).astype(jnp.bfloat16)
    flat = jnp.transpose(slip.reshape(RUP_SLOTS, rows, variations, BLK * TAPS), (0, 2, 1, 3))
    flat = flat.reshape(RUP_SLOTS * variations, full)
    left = jnp.dot(flat, move, preferred_element_type=jnp.bfloat16)
    left = left.reshape(RUP_SLOTS, variations, full)

    share = variations // workers
    partial_value = pl.pallas_call(
        functools.partial(conv_kernel, rows, variations, samples, workers),
        out_shape=jax.ShapeDtypeStruct((workers, RUP_SLOTS, 3, share, samples), jnp.bfloat16),
        in_specs=[pl.BlockSpec(memory_space=pltpu.VMEM)] * 2,
        out_specs=pl.BlockSpec(memory_space=pltpu.VMEM),
        scratch_shapes=[pltpu.VMEM((INNER * BLK * rows, samples), jnp.bfloat16)],
        compiler_params=pltpu.CompilerParams(vmem_limit_bytes=40 * 1024 * 1024),
    )(blocks, left)
    swapped = lax.all_to_all(partial_value, "worker", split_axis=0, concat_axis=0, tiled=True)
    total = jnp.sum(swapped.astype(jnp.float32), axis=0)
    return jnp.transpose(total, (0, 2, 1, 3))


def solution(mesh):
    return jax.shard_map(
        functools.partial(local, mesh.shape["worker"]),
        mesh=mesh,
        in_specs=(
            P(("site", "handler", "worker"), None, None, None),
            P(None, ("handler", "worker")),
            P(("site", "handler", "worker"), None),
            P(("site", "handler", "worker")),
            P(("site", "handler", "worker"), None, None),
        ),
        out_specs=P(("site", "handler"), "worker", None, None),
        check_vma=False,
    )
```

```python
import functools
import jax
import jax.numpy as jnp
from jax import lax
from jax.experimental import pallas as pl
from jax.experimental.pallas import tpu as pltpu
from jax.sharding import PartitionSpec as P

TAPS = 64
BLK = 2
RUP_SLOTS = 4
OUTER = 4
INNER = TAPS // OUTER


def green_kernel(mech_ref, sgt_ref, out_ref):
    comps, parts, _, samples = sgt_ref.shape
    for k in range(parts):
        total = mech_ref[:, 0:1] * sgt_ref[0, k].astype(jnp.float32)
        for comp in range(1, comps):
            total = total + mech_ref[:, comp : comp + 1] * sgt_ref[comp, k].astype(jnp.float32)
        out_ref[:, k * samples : (k + 1) * samples] = total.astype(jnp.bfloat16)


def combine_points(sgt, mechanism):
    points, comps, parts, samples = sgt.shape
    group = min(16, points)
    return pl.pallas_call(
        green_kernel,
        grid=(points // group,),
        out_shape=jax.ShapeDtypeStruct((points, parts * samples), jnp.bfloat16),
        in_specs=[
            pl.BlockSpec((group, comps), lambda g: (g, 0)),
            pl.BlockSpec((comps, parts, group, samples), lambda g: (0, 0, g, 0)),
        ],
        out_specs=pl.BlockSpec((group, parts * samples), lambda g: (g, 0)),
        cost_estimate=pl.CostEstimate(
            flops=12 * sgt.size, bytes_accessed=4 * sgt.size, transcendentals=0
        ),
    )(mechanism.astype(jnp.float32).T, jnp.transpose(sgt, (1, 2, 0, 3)))


def conv_kernel(rows, variations, samples, workers, blk_ref, slip_ref, out_ref, shift_ref):
    depth = INNER * BLK * rows
    share = variations // workers
    lane = lax.broadcasted_iota(jnp.int32, (BLK * rows, samples), 1)
    wide = lax.broadcasted_iota(jnp.int32, (variations, samples), 1)

    def slot_step(slot, carry):
        left = jnp.concatenate(
            [slip_ref[slot, :, a * depth : (a + 1) * depth] for a in range(OUTER)], axis=0
        )
        for k in range(3):
            x = blk_ref[slot, :, k * samples : (k + 1) * samples].astype(jnp.float32)
            for b in range(INNER):
                moved = x if b == 0 else jnp.where(lane >= b, pltpu.roll(x, b, 1), 0.0)
                shift_ref[b * BLK * rows : (b + 1) * BLK * rows, :] = moved.astype(jnp.bfloat16)
            y = jnp.dot(left, shift_ref[...], preferred_element_type=jnp.float32)
            total = y[:variations]
            for a in range(1, OUTER):
                part = pltpu.roll(y[a * variations : (a + 1) * variations], a * INNER, 1)
                total = total + jnp.where(wide >= a * INNER, part, 0.0)
            total = total.astype(jnp.bfloat16)
            for w in range(workers):
                out_ref[w, slot, k] = total[w * share : (w + 1) * share]
        return carry

    lax.fori_loop(0, RUP_SLOTS, slot_step, 0)


def local(workers, sgt, mechanism, req_owner, req_local, slip):
    peers = lax.axis_size(("handler", "worker"))
    samples = sgt.shape[-1]
    requests = req_local.shape[0]
    rows = requests // RUP_SLOTS
    variations = slip.shape[1]
    capacity = max(2, (2 * requests + peers - 1) // peers)
    owner = req_owner[:, 0]
    order = jnp.arange(requests)
    same = (owner[:, None] == owner[None, :]) & (order[:, None] > order[None, :])
    position = owner * capacity + jnp.sum(same.astype(jnp.int32), axis=1)
    places = jnp.arange(peers * capacity, dtype=jnp.int32)
    table = jnp.sum(
        jnp.where(position[:, None] == places[None, :], req_local[:, None], 0), axis=0
    )
    asked = lax.all_to_all(
        table.reshape(peers, capacity),
        ("handler", "worker"),
        split_axis=0,
        concat_axis=0,
        tiled=True,
    )
    green_here = combine_points(sgt, mechanism)
    point = jnp.arange(BLK, dtype=jnp.int32)
    picked = asked.reshape(-1)[:, None] * BLK + point[None, :]
    chosen = green_here[picked.reshape(-1)].reshape(peers, capacity * BLK, 3 * samples)
    arrived = lax.all_to_all(
        chosen, ("handler", "worker"), split_axis=0, concat_axis=0, tiled=True
    )
    taken = position.reshape(RUP_SLOTS, 1, rows) * BLK + point[None, :, None]
    blocks = arrived.reshape(peers * capacity * BLK, 3 * samples)[taken.reshape(-1)]
    blocks = blocks.reshape(RUP_SLOTS, BLK * rows, 3 * samples)

    full = rows * BLK * TAPS
    src = jnp.arange(full, dtype=jnp.int32)
    dst_of = (
        (src % TAPS) * (BLK * rows) + (src // TAPS) % BLK * rows + src // (TAPS * BLK)
    )
    move = (dst_of[:, None] == src[None, :]).astype(jnp.bfloat16)
    flat = jnp.transpose(slip.reshape(RUP_SLOTS, rows, variations, BLK * TAPS), (0, 2, 1, 3))
    flat = flat.reshape(RUP_SLOTS * variations, full)
    left = jnp.dot(flat, move, preferred_element_type=jnp.bfloat16)
    left = left.reshape(RUP_SLOTS, variations, full)

    share = variations // workers
    partial_value = pl.pallas_call(
        functools.partial(conv_kernel, rows, variations, samples, workers),
        out_shape=jax.ShapeDtypeStruct((workers, RUP_SLOTS, 3, share, samples), jnp.bfloat16),
        in_specs=[pl.BlockSpec(memory_space=pltpu.VMEM)] * 2,
        out_specs=pl.BlockSpec(memory_space=pltpu.VMEM),
        scratch_shapes=[pltpu.VMEM((INNER * BLK * rows, samples), jnp.bfloat16)],
        compiler_params=pltpu.CompilerParams(vmem_limit_bytes=40 * 1024 * 1024),
    )(blocks, left)
    swapped = lax.all_to_all(partial_value, "worker", split_axis=0, concat_axis=0, tiled=True)
    total = jnp.sum(swapped.astype(jnp.float32), axis=0)
    return jnp.transpose(total, (0, 2, 1, 3))


def solution(mesh):
    return jax.shard_map(
        functools.partial(local, mesh.shape["worker"]),
        mesh=mesh,
        in_specs=(
            P(("site", "handler", "worker"), None, None, None),
            P(None, ("handler", "worker")),
            P(("site", "handler", "worker"), None),
            P(("site", "handler", "worker")),
            P(("site", "handler", "worker"), None, None),
        ),
        out_specs=P(("site", "handler"), "worker", None, None),
        check_vma=False,
    )
```
